32 devices in a mesh: row: 2 (over x), col: 4 (over y, core), layer: 4 (over z).
Axes of the slice: x: 2, y: 2, z: 4, core: 2. Of those that a mesh axis runs over, the one named last changes fastest.
Arguments:
- object_field: float32 [2, 512, 1024], P(None, 'row', 'col'), may hold values from -6 to 6
- probe_modes: float32 [2, 4, 256, 256], replicated, may hold values from -6 to 6
- amplitudes: float32 [32, 256, 256], P(('row', 'col', 'layer')), may hold values from 0 to 4
- offsets: int32 [32, 2], P(('row', 'col', 'layer')), may hold values from 0 to 768, as said below
Outputs:
- new_object: float32 [2, 512, 1024], P(None, 'row', 'col')
The draws below stay inside these ranges and needn't reach their ends.
Inputs may be any that keep to these rules, and one draw needn't show every extreme that they name: `offsets`: every patch lies inside the 512 x 1024 object. A position held by the device at tile (r, c) has its corner inside that tile: rows r * 256 to (r + 1) * 256 - 1 and columns c * 256 to (c + 1) * 256 - 1. On a device whose tile row is not the last, its first position's patch reaches into the next tile row.
All inputs are finite; a program needn't handle non-finite values.
Results may differ from the reference program's by a relative error of at most 0.0001.
Values sent between devices are 32-bit elements; how exact they have to be, the bound alone decides.
A program may use at most 64 MiB of HBM per device.

```python
import jax
import jax.numpy as jnp
from jax import lax

PATCH = 256
MODES = 4
TILE_R = 256
TILE_C = 256
POS_DEV = 1
OBJ_R = 512
OBJ_C = 1024
POSITIONS = 32
N_ROW = 2
N_COL = 4
N_LAYER = 4


def draw_offsets(key, part):
    index = jnp.arange(POSITIONS, dtype=jnp.int32)
    device = index // POS_DEV
    slot = index % POS_DEV
    tile_row = device // (N_COL * N_LAYER)
    tile_col = device // N_LAYER % N_COL
    key_rows, key_cols = jax.random.split(jax.random.fold_in(key, 17))
    rows_high = jnp.where(tile_row == N_ROW - 1, TILE_R - PATCH + 1, TILE_R)
    rows_low = jnp.where((slot == 0) & (tile_row < N_ROW - 1), TILE_R - PATCH + 1, 0)
    draw_rows = jax.random.randint(key_rows, (POSITIONS,), 0, 1 << 30, dtype=jnp.int32)
    local_rows = rows_low + draw_rows % (rows_high - rows_low)
    cols_high = jnp.where(tile_col == N_COL - 1, TILE_C - PATCH + 1, TILE_C)
    draw_cols = jax.random.randint(key_cols, (POSITIONS,), 0, 1 << 30, dtype=jnp.int32)
    local_cols = draw_cols % cols_high
    return jnp.stack([tile_row * TILE_R + local_rows, tile_col * TILE_C + local_cols], axis=-1).astype(jnp.int32)


def steps_of(stream_key, shape, cuts, low, top_value):
    level = 1.0
    for axis_at, parts in cuts:
        draws = jax.random.uniform(jax.random.fold_in(jax.random.fold_in(stream_key, 6), axis_at), (parts,), jnp.float32, low / len(cuts), top_value / len(cuts))
        level = level * jnp.repeat(jnp.exp(draws), shape[axis_at] // parts).reshape((-1,) + (1,) * (len(shape) - 1 - axis_at))
    return level


def centred(rng, shape, spread, most, shards=(), kind=jnp.bfloat16):
    entries = jax.random.normal(rng, shape, jnp.float32) * spread
    if len(shards) > 0:
        entries = steps_of(rng, shape, shards, -0.22, 0.18) * entries
    return jnp.clip(entries, min=-most, max=most).astype(kind)


def setup_inputs(seed: int = 0) -> dict:
    seeds = jax.random.split(jax.random.key(seed), 5)
    return {
        "object_field": centred(seeds[0], (2, OBJ_R, OBJ_C), 1.0, 6.0, ((1, 2), (2, 4)), jnp.float32),
        "probe_modes": centred(seeds[1], (2, MODES, PATCH, PATCH), 1.0, 6.0, (), jnp.float32),
        "amplitudes": jnp.clip(4.0 * jax.random.uniform(seeds[2], (POSITIONS, PATCH, PATCH), jnp.float32) ** steps_of(seeds[2], (POSITIONS, PATCH, PATCH), ((0, 32),), -0.2, 0.2), 0.0, 4.0),
        "offsets": draw_offsets(jax.random.fold_in(seeds[4], 71), 0),
    }


SOFTEN = 0.05
DAMPING = 0.5

def reference(object_field, probe_modes, amplitudes, offsets):
    probe = lax.complex(probe_modes[0], probe_modes[1])
    power = lax.optimization_barrier(jnp.sum(probe_modes[0] * probe_modes[0] + probe_modes[1] * probe_modes[1], axis=0))
    zero_index = jnp.int32(0)

    def one_position(index, carry):
        numer, denom = carry
        row_at = offsets[index, 0].astype(jnp.int32)
        col_at = offsets[index, 1].astype(jnp.int32)
        patch = lax.dynamic_slice(object_field, (zero_index, row_at, col_at), (2, PATCH, PATCH))
        exit_wave = probe * lax.complex(patch[0], patch[1])[None]
        far = jnp.fft.fft2(exit_wave, norm='ortho')
        intensity = lax.optimization_barrier(jnp.sum(far.real * far.real + far.imag * far.imag, axis=0))
        ratio = amplitudes[index] / (jnp.sqrt(intensity) + SOFTEN)
        revised = jnp.fft.ifft2(far * ratio[None], norm='ortho')
        contrib = lax.optimization_barrier(jnp.sum(jnp.conj(probe) * revised, axis=0))
        block = jnp.stack([contrib.real, contrib.imag])
        old_block = lax.dynamic_slice(numer, (zero_index, row_at, col_at), (2, PATCH, PATCH))
        numer = lax.dynamic_update_slice(numer, old_block + block, (zero_index, row_at, col_at))
        old_power = lax.dynamic_slice(denom, (row_at, col_at), (PATCH, PATCH))
        denom = lax.dynamic_update_slice(denom, old_power + power, (row_at, col_at))
        return (numer, denom)
    numer0 = jnp.zeros(object_field.shape, jnp.float32)
    denom0 = jnp.zeros(object_field.shape[1:], jnp.float32)
    numer, denom = lax.fori_loop(0, POSITIONS, one_position, (numer0, denom0))
    return (numer + DAMPING * object_field) / (denom + DAMPING)[None]
```

```python
import functools

import jax
import jax.numpy as jnp
import numpy as np
from jax import lax
from jax.experimental import pallas as pl
from jax.experimental.pallas import tpu as pltpu
from jax.sharding import PartitionSpec as P

SOFTEN = 0.05
DAMPING = 0.5
AXES = ("row", "col", "layer")
PIECES = 4


def place():
    return tuple(lax.axis_index(a) for a in AXES)


def send(src, dst, send_sem, recv_sem, device):
    return pltpu.make_async_remote_copy(
        src_ref=src,
        dst_ref=dst,
        send_sem=send_sem,
        recv_sem=recv_sem,
        device_id=device,
        device_id_type=pl.DeviceIdType.MESH,
    )


def greet(rows, cols, layers):
    r, c, l = place()
    barrier = pltpu.get_barrier_semaphore()

    def tell(device):
        pl.semaphore_signal(
            barrier, inc=1, device_id=device, device_id_type=pl.DeviceIdType.MESH
        )

    near = (
        (c > 0, (r, c - 1, l)),
        (c < cols - 1, (r, c + 1, l)),
        (r > 0, (r - 1, c, l)),
        (r < rows - 1, (r + 1, c, l)),
    )
    for there, device in near:
        pl.when(there)(functools.partial(tell, device))
    for d in range(1, layers):
        tell((r, c, lax.rem(l + d, layers)))
    count = layers - 1
    for there, _ in near:
        count += there.astype(jnp.int32)
    pl.semaphore_wait(barrier, count)


def halo_kernel(
    sizes, corner, obj, off, merged, offs, right, below, diag,
    s_right, r_right, s_below, r_below, s_diag, r_diag, s_off, r_off, s_pass, r_pass,
):
    rows, cols, layers = sizes
    side = obj.shape[1]
    step = side // PIECES
    r, c, l = place()
    has_right, has_left = c < cols - 1, c > 0
    has_below, has_above = r < rows - 1, r > 0
    greet(rows, cols, layers)

    def piece(ref, k):
        return ref.at[:, pl.ds(k * step, step), :]

    to_left = send(obj, right, s_right, r_right, (r, c - 1, l))
    pl.when(has_left)(to_left.start)
    ups = [
        send(piece(obj, k), piece(below, k), s_below.at[k], r_below.at[k], (r - 1, c, l))
        for k in range(PIECES)
    ]
    for up in ups:
        pl.when(has_above)(up.start)
    mine = offs.at[0, pl.ds(l, 1)]
    peers = [
        send(off, mine, s_off.at[d], r_off.at[d], (r, c, lax.rem(l + d, layers)))
        for d in range(1, layers)
    ]
    for peer in peers:
        peer.start()
    offs[0, pl.ds(l, 1)] = off[...]
    for peer in peers:
        peer.wait()
    across = send(offs.at[0], offs.at[1], s_pass.at[0], r_pass.at[0], (r, c + 1, l))
    pl.when(has_right)(across.start)

    diags = [
        send(piece(below, k), piece(diag, k), s_diag.at[k], r_diag.at[k], (r, c - 1, l))
        for k in range(PIECES)
    ]

    def forward(k):
        @pl.when(has_below)
        def _():
            ups[k].wait_recv()
            pl.when(has_left)(diags[k].start)

    forward(0)
    down0 = send(offs.at[0], offs.at[2], s_pass.at[1], r_pass.at[1], (r + 1, c, l))
    down1 = send(offs.at[1], offs.at[3], s_pass.at[2], r_pass.at[2], (r + 1, c, l))
    pl.when(has_left)(across.wait_recv)

    @pl.when(has_below)
    def _():
        down0.start()
        pl.when(has_left)(down1.start)

    for k in range(1, PIECES):
        forward(k)

    base_row, base_col = corner[0, 0] - r * side, corner[0, 1] - c * side
    pl.when(has_right)(to_left.wait_recv)
    lane = lax.broadcasted_iota(jnp.int32, (step, side), 1)
    line = lax.broadcasted_iota(jnp.int32, (step, side), 0)
    for k in range(PIECES):
        part = pl.ds(k * step, step)
        for h in range(2):
            merged[h, part, :] = obj[h, part, :]

        @pl.when(has_right)
        def _():
            for h in range(2):
                merged[h, part, :] = jnp.where(
                    lane < base_col, right[h, part, :], merged[h, part, :]
                )

        @pl.when(has_below)
        def _():
            for h in range(2):
                merged[h, part, :] = jnp.where(
                    (line + k * step < base_row) & (lane >= base_col),
                    below[h, part, :],
                    merged[h, part, :],
                )

        @pl.when(has_below & has_right)
        def _():
            diags[k].wait_recv()
            for h in range(2):
                merged[h, part, :] = jnp.where(
                    (line + k * step < base_row) & (lane < base_col),
                    diag[h, part, :],
                    merged[h, part, :],
                )

    @pl.when(jnp.logical_not(has_left))
    def _():
        offs[1] = jnp.zeros(offs.shape[1:], jnp.int32)

    @pl.when(jnp.logical_not(has_above))
    def _():
        offs[2] = jnp.zeros(offs.shape[1:], jnp.int32)

    @pl.when(jnp.logical_not(has_above & has_left))
    def _():
        offs[3] = jnp.zeros(offs.shape[1:], jnp.int32)

    pl.when(has_left)(to_left.wait_send)
    pl.when(has_right)(across.wait_send)

    @pl.when(has_above)
    def _():
        for up in ups:
            up.wait_send()
        down0.wait_recv()
        pl.when(has_left)(down1.wait_recv)

    @pl.when(has_below)
    def _():
        down0.wait_send()

        @pl.when(has_left)
        def _():
            down1.wait_send()
            for copy in diags:
                copy.wait_send()


def split(x):
    high = x.astype(jnp.bfloat16)
    return high, (x - high.astype(jnp.float32)).astype(jnp.bfloat16)


def prod(left, right):
    def one(a, b):
        return jnp.dot(a, b, preferred_element_type=jnp.float32)

    return one(left[0], right[0]) + (one(left[0], right[1]) + one(left[1], right[0]))


def wave_kernel(
    sizes, corner, offs, merged, probe, amp, fwd_high, fwd_low, inv_high, inv_low,
    terms, weight, rolled, far, ratio, power, twice,
):
    layers = sizes[2]
    share = merged.shape[1] // layers
    side = merged.shape[1]
    modes = probe.shape[1]
    r, c, l = place()
    has_left, has_above = c > 0, r > 0
    down, over = corner[0, 0] - r * side, corner[0, 1] - c * side
    fwd = (fwd_high, fwd_low)
    inv = (inv_high, inv_low)

    def last(x, table):
        return prod(split(x), (table[0][...], table[1][...]))

    def first(table, x):
        a = (table[0][:, :side], table[1][:, :side])
        b = (table[0][:, side:], table[1][:, side:])
        return prod(a, split(x[:, :side])) + prod(b, split(x[:, side:]))

    ratio[...] = jnp.zeros_like(ratio)
    power[...] = jnp.zeros_like(power)

    def forward(m, carry):
        plain = probe[0, m], probe[1, m]
        power[...] += plain[0] * plain[0] + plain[1] * plain[1]
        real, imag = (pltpu.roll(pltpu.roll(x, down, 0), over, 1) for x in plain)
        rolled[0, m] = real
        rolled[1, m] = imag
        exit_wave = jnp.concatenate(
            [real * merged[0] - imag * merged[1], real * merged[1] + imag * merged[0]], axis=1
        )
        spread = first(inv, last(exit_wave, fwd))
        far[m] = spread
        ratio[...] += spread[:side] * spread[:side] + spread[side:] * spread[side:]
        return carry

    lax.fori_loop(0, modes, forward, 0)
    ratio[...] = amp[0] / (jnp.sqrt(ratio[...]) + SOFTEN)
    terms[...] = jnp.zeros_like(terms)

    def backward(m, carry):
        scale = ratio[...]
        fixed = jnp.concatenate([far[m, :side] * scale, far[m, side:] * scale], axis=1)
        back = first(fwd, fixed)
        back = last(jnp.concatenate([back[:side], back[side:]], axis=1), inv)
        new_real, new_imag = back[:, :side], back[:, side:]
        real, imag = rolled[0, m], rolled[1, m]
        terms[0] += real * new_real + imag * new_imag
        terms[1] += real * new_imag - imag * new_real
        return carry

    lax.fori_loop(0, modes, backward, 0)

    twice[:side, :] = power[...]
    twice[side : 2 * side, :] = power[...]
    twice[2 * side :, :] = jnp.zeros((8, side), jnp.float32)
    lane = lax.broadcasted_iota(jnp.int32, (share, side), 1)
    at = lax.broadcasted_iota(jnp.int32, (share, side), 0) + l * share
    total = jnp.zeros((share, side), jnp.float32)
    there = (None, has_left, has_above, has_left & has_above)
    for group in range(4):
        for layer in range(layers):
            a, b = corner_of(offs, group, layer, side)
            a = jnp.clip(a, 0, side)
            b = jnp.clip(b, 0, side)
            start = side + l * share - a
            extra = lax.rem(start, 8)
            window = twice[pl.ds(pl.multiple_of(start - extra, 8), share + 8), :]
            window = pltpu.roll(window, lax.rem(share + 8 - extra, share + 8), 0)[:share]
            window = pltpu.roll(window, lax.rem(b, side), 1)
            keep = (at < a) if group >= 2 else (at >= a)
            keep &= (lane < b) if group % 2 else (lane >= b)
            if there[group] is not None:
                keep &= there[group]
            total += jnp.where(keep, window, 0.0)
    weight[...] = total + DAMPING


def corner_of(offs, group, layer, side):
    r, c, _ = place()
    tile_row = r - (1 if group >= 2 else 0)
    tile_col = c - (group % 2)
    return offs[group, layer, 0] - tile_row * side, offs[group, layer, 1] - tile_col * side


def sum_kernel(
    sizes, offs, terms, weight, obj, out,
    left, own, lower, upper, shares, s_left, r_left, s_down, r_down, s_rs, r_rs, s_ag, r_ag,
):
    rows, cols, layers = sizes
    side = obj.shape[1]
    step = side // PIECES
    share = side // layers
    r, c, l = place()
    has_right, has_left = c < cols - 1, c > 0
    has_below, has_above = r < rows - 1, r > 0
    greet(rows, cols, layers)

    def piece(ref, k):
        return ref.at[:, pl.ds(k * step, step), :]

    rights = [
        send(piece(terms, k), piece(left, k), s_left.at[k], r_left.at[k], (r, c + 1, l))
        for k in range(PIECES)
    ]
    for copy in rights:
        pl.when(has_right)(copy.start)
    downs = [
        send(piece(lower, k), piece(upper, k), s_down.at[k], r_down.at[k], (r + 1, c, l))
        for k in range(PIECES)
    ]
    spreads = []
    for d in range(1, layers):
        peer = lax.rem(l + d, layers)
        spreads.append(
            (
                peer,
                send(
                    own.at[:, pl.ds(peer * share, share), :],
                    shares.at[d],
                    s_rs.at[d],
                    r_rs.at[d],
                    (r, c, peer),
                ),
            )
        )

    lane = lax.broadcasted_iota(jnp.int32, (step, side), 1)
    line = lax.broadcasted_iota(jnp.int32, (step, side), 0)
    down, over = corner_of(offs, 0, l, side)
    left_down, left_over = corner_of(offs, 1, l, side)
    for k in range(PIECES):
        part = pl.ds(k * step, step)
        at = line + k * step
        for h in range(2):
            mine = jnp.where(lane >= over, terms[h, part, :], 0.0)
            own[h, part, :] = jnp.where(at >= down, mine, 0.0)
            lower[h, part, :] = jnp.where(at < down, mine, 0.0)

        @pl.when(has_left)
        def _():
            rights[k].wait_recv()
            for h in range(2):
                other = jnp.where(lane < left_over, left[h, part, :], 0.0)
                own[h, part, :] += jnp.where(at >= left_down, other, 0.0)
                lower[h, part, :] += jnp.where(at < left_down, other, 0.0)

        pl.when(has_below)(downs[k].start)

        @pl.when(jnp.logical_not(has_above))
        def _():
            for peer, copy in spreads:
                pl.when(peer * share // step == k)(copy.start)

    @pl.when(has_above)
    def _():
        for k in range(PIECES):
            part = pl.ds(k * step, step)
            downs[k].wait_recv()
            for h in range(2):
                own[h, part, :] += upper[h, part, :]
            for peer, copy in spreads:
                pl.when(peer * share // step == k)(copy.start)

    strip = pl.ds(pl.multiple_of(l * share, share), share)
    for _, copy in spreads:
        copy.wait_recv()
    for h in range(2):
        number = own[h, strip, :] + DAMPING * obj[h, strip, :]
        for d in range(1, layers):
            number += shares[d, h]
        out[h, strip, :] = number / weight[...]
    gathers = [
        send(
            out.at[:, strip, :],
            out.at[:, strip, :],
            s_ag.at[d],
            r_ag.at[d],
            (r, c, lax.rem(l + d, layers)),
        )
        for d in range(1, layers)
    ]
    for copy in gathers:
        copy.start()
    for copy in gathers:
        copy.wait()
    for _, copy in spreads:
        copy.wait_send()

    @pl.when(has_right)
    def _():
        for copy in rights:
            copy.wait_send()

    @pl.when(has_below)
    def _():
        for copy in downs:
            copy.wait_send()


def tables(side):
    steps = np.arange(side)
    angle = (steps[:, None] * steps[None, :] % side) * (2.0 * np.pi / side)
    real, imag = np.cos(angle) / np.sqrt(side), -np.sin(angle) / np.sqrt(side)
    both = np.block([[real, imag], [-imag, real]])

    def halves(x):
        x = x.astype(np.float32)
        high = x.astype(jnp.bfloat16)
        return high, (x - high.astype(np.float32)).astype(jnp.bfloat16)

    return halves(both) + halves(both.T)


def body(sizes, object_field, probe_modes, amplitudes, offsets):
    rows, cols, layers = sizes
    side = object_field.shape[1]
    assert object_field.shape[2] == side and probe_modes.shape[2] == side
    assert offsets.shape[0] == 1 and side % (8 * layers) == 0
    modes = probe_modes.shape[1]
    vmem = pl.BlockSpec(memory_space=pltpu.VMEM)
    smem = pl.BlockSpec(memory_space=pltpu.SMEM)
    pair = (2, side, side)
    f32 = jnp.float32
    dma = pltpu.SemaphoreType.DMA
    off = jnp.pad(offsets.reshape(1, 1, 2), ((0, 0), (0, 0), (0, 126)))
    off = jnp.broadcast_to(off, (1, 8, 128))
    merged, offs = pl.pallas_call(
        functools.partial(halo_kernel, sizes),
        out_shape=(
            jax.ShapeDtypeStruct(pair, f32),
            jax.ShapeDtypeStruct((4, layers, 8, 128), jnp.int32),
        ),
        in_specs=[smem, vmem, vmem],
        out_specs=(vmem, vmem),
        scratch_shapes=[pltpu.VMEM(pair, f32)] * 3
        + [dma(()), dma(())]
        + [dma((PIECES,))] * 4
        + [dma((layers,))] * 2
        + [dma((3,))] * 2,
        compiler_params=pltpu.CompilerParams(collective_id=0, has_side_effects=True),
        name="halo",
    )(offsets, object_field, off)
    corners = offs[:, :, 0, :2]
    terms, weight = pl.pallas_call(
        functools.partial(wave_kernel, sizes),
        out_shape=(
            jax.ShapeDtypeStruct(pair, f32),
            jax.ShapeDtypeStruct((side // layers, side), f32),
        ),
        in_specs=[smem, smem] + [vmem] * 7,
        out_specs=(vmem, vmem),
        scratch_shapes=[
            pltpu.VMEM((2, modes, side, side), f32),
            pltpu.VMEM((modes, 2 * side, side), f32),
            pltpu.VMEM((side, side), f32),
            pltpu.VMEM((side, side), f32),
            pltpu.VMEM((2 * side + 8, side), f32),
        ],
        name="wave",
    )(offsets, corners, merged, probe_modes, amplitudes, *(jnp.asarray(t) for t in tables(side)))
    return pl.pallas_call(
        functools.partial(sum_kernel, sizes),
        out_shape=jax.ShapeDtypeStruct(pair, f32),
        in_specs=[smem] + [vmem] * 3,
        out_specs=vmem,
        scratch_shapes=[pltpu.VMEM(pair, f32)] * 4
        + [pltpu.VMEM((layers, 2, side // layers, side), f32)]
        + [dma((PIECES,))] * 4
        + [dma((layers,))] * 4,
        compiler_params=pltpu.CompilerParams(collective_id=1, has_side_effects=True),
        name="sums",
    )(corners, terms, weight, object_field)


def solution(mesh):
    sizes = tuple(mesh.shape[a] for a in AXES)
    placed = (
        P(None, "row", "col"),
        P(),
        P(("row", "col", "layer"), None, None),
        P(("row", "col", "layer"), None),
    )
    return jax.shard_map(
        functools.partial(body, sizes),
        mesh=mesh,
        in_specs=placed,
        out_specs=P(None, "row", "col"),
        check_vma=False,
    )
```

```python
import functools

import jax
import jax.numpy as jnp
import numpy as np
from jax import lax
from jax.experimental import pallas as pl
from jax.experimental.pallas import tpu as pltpu
from jax.sharding import PartitionSpec as P

SOFTEN = 0.05
DAMPING = 0.5
AXES = ("row", "col", "layer")
PIECES = 4


def place():
    return tuple(lax.axis_index(a) for a in AXES)


def send(src, dst, send_sem, recv_sem, device):
    return pltpu.make_async_remote_copy(
        src_ref=src,
        dst_ref=dst,
        send_sem=send_sem,
        recv_sem=recv_sem,
        device_id=device,
        device_id_type=pl.DeviceIdType.MESH,
    )


def greet(rows, cols, layers):
    r, c, l = place()
    barrier = pltpu.get_barrier_semaphore()

    def tell(device):
        pl.semaphore_signal(
            barrier, inc=1, device_id=device, device_id_type=pl.DeviceIdType.MESH
        )

    near = (
        (c > 0, (r, c - 1, l)),
        (c < cols - 1, (r, c + 1, l)),
        (r > 0, (r - 1, c, l)),
        (r < rows - 1, (r + 1, c, l)),
    )
    for there, device in near:
        pl.when(there)(functools.partial(tell, device))
    for d in range(1, layers):
        tell((r, c, lax.rem(l + d, layers)))
    count = layers - 1
    for there, _ in near:
        count += there.astype(jnp.int32)
    pl.semaphore_wait(barrier, count)


def halo_kernel(
    sizes, corner, obj, merged, offs, right, below, diag,
    s_right, r_right, s_below, r_below, s_diag, r_diag, s_off, r_off, s_pass, r_pass,
):
    rows, cols, layers = sizes
    side = obj.shape[1]
    step = side // PIECES
    r, c, l = place()
    has_right, has_left = c < cols - 1, c > 0
    has_below, has_above = r < rows - 1, r > 0
    at = lax.broadcasted_iota(jnp.int32, (1, 1, 128), 2)
    offs[0, pl.ds(l, 1)] = jnp.where(at == 0, corner[0, 0], corner[0, 1])
    greet(rows, cols, layers)

    def piece(ref, k):
        return ref.at[:, pl.ds(k * step, step), :]

    to_left = send(obj, right, s_right, r_right, (r, c - 1, l))
    pl.when(has_left)(to_left.start)
    ups = [
        send(piece(obj, k), piece(below, k), s_below.at[k], r_below.at[k], (r - 1, c, l))
        for k in range(PIECES)
    ]
    for up in ups:
        pl.when(has_above)(up.start)
    mine = offs.at[0, pl.ds(l, 1)]
    peers = [
        send(mine, mine, s_off.at[d], r_off.at[d], (r, c, lax.rem(l + d, layers)))
        for d in range(1, layers)
    ]
    for peer in peers:
        peer.start()
    for peer in peers:
        peer.wait()
    across = send(offs.at[0], offs.at[1], s_pass.at[0], r_pass.at[0], (r, c + 1, l))
    pl.when(has_right)(across.start)

    diags = [
        send(piece(below, k), piece(diag, k), s_diag.at[k], r_diag.at[k], (r, c - 1, l))
        for k in range(PIECES)
    ]

    def forward(k):
        @pl.when(has_below)
        def _():
            ups[k].wait_recv()
            pl.when(has_left)(diags[k].start)

    forward(0)
    down0 = send(offs.at[0], offs.at[2], s_pass.at[1], r_pass.at[1], (r + 1, c, l))
    down1 = send(offs.at[1], offs.at[3], s_pass.at[2], r_pass.at[2], (r + 1, c, l))
    pl.when(has_left)(across.wait_recv)

    @pl.when(has_below)
    def _():
        down0.start()
        pl.when(has_left)(down1.start)

    for k in range(1, PIECES):
        forward(k)

    base_row, base_col = corner[0, 0] - r * side, corner[0, 1] - c * side
    pl.when(has_right)(to_left.wait_recv)
    lane = lax.broadcasted_iota(jnp.int32, (step, side), 1)
    line = lax.broadcasted_iota(jnp.int32, (step, side), 0)
    for k in range(PIECES):
        part = pl.ds(k * step, step)
        for h in range(2):
            merged[h, part, :] = obj[h, part, :]

        @pl.when(has_right)
        def _():
            for h in range(2):
                merged[h, part, :] = jnp.where(
                    lane < base_col, right[h, part, :], merged[h, part, :]
                )

        @pl.when(has_below)
        def _():
            for h in range(2):
                merged[h, part, :] = jnp.where(
                    (line + k * step < base_row) & (lane >= base_col),
                    below[h, part, :],
                    merged[h, part, :],
                )

        @pl.when(has_below & has_right)
        def _():
            diags[k].wait_recv()
            for h in range(2):
                merged[h, part, :] = jnp.where(
                    (line + k * step < base_row) & (lane < base_col),
                    diag[h, part, :],
                    merged[h, part, :],
                )

    @pl.when(jnp.logical_not(has_left))
    def _():
        offs[1] = jnp.zeros(offs.shape[1:], jnp.int32)

    @pl.when(jnp.logical_not(has_above))
    def _():
        offs[2] = jnp.zeros(offs.shape[1:], jnp.int32)

    @pl.when(jnp.logical_not(has_above & has_left))
    def _():
        offs[3] = jnp.zeros(offs.shape[1:], jnp.int32)

    pl.when(has_left)(to_left.wait_send)
    pl.when(has_right)(across.wait_send)

    @pl.when(has_above)
    def _():
        for up in ups:
            up.wait_send()
        down0.wait_recv()
        pl.when(has_left)(down1.wait_recv)

    @pl.when(has_below)
    def _():
        down0.wait_send()

        @pl.when(has_left)
        def _():
            down1.wait_send()
            for copy in diags:
                copy.wait_send()


def split(x):
    high = x.astype(jnp.bfloat16)
    return high, (x - high.astype(jnp.float32)).astype(jnp.bfloat16)


def prod(left, right):
    def one(a, b):
        return jnp.dot(a, b, preferred_element_type=jnp.float32)

    return one(left[0], right[0]) + (one(left[0], right[1]) + one(left[1], right[0]))


def wave_kernel(
    sizes, corner, offs, merged, probe, amp, fwd_high, fwd_low, inv_high, inv_low,
    terms, weight, rolled, far, ratio, power, twice,
):
    layers = sizes[2]
    share = merged.shape[1] // layers
    side = merged.shape[1]
    modes = probe.shape[1]
    r, c, l = place()
    has_left, has_above = c > 0, r > 0
    down, over = corner[0, 0] - r * side, corner[0, 1] - c * side
    fwd = (fwd_high, fwd_low)
    inv = (inv_high, inv_low)

    def last(x, table):
        return prod(split(x), (table[0][...], table[1][...]))

    def first(table, x):
        a = (table[0][:, :side], table[1][:, :side])
        b = (table[0][:, side:], table[1][:, side:])
        return prod(a, split(x[:, :side])) + prod(b, split(x[:, side:]))

    ratio[...] = jnp.zeros_like(ratio)
    power[...] = jnp.zeros_like(power)

    def forward(m, carry):
        plain = probe[0, m], probe[1, m]
        power[...] += plain[0] * plain[0] + plain[1] * plain[1]
        real, imag = (pltpu.roll(pltpu.roll(x, down, 0), over, 1) for x in plain)
        rolled[0, m] = real
        rolled[1, m] = imag
        exit_wave = jnp.concatenate(
            [real * merged[0] - imag * merged[1], real * merged[1] + imag * merged[0]], axis=1
        )
        spread = first(inv, last(exit_wave, fwd))
        far[m] = spread
        ratio[...] += spread[:side] * spread[:side] + spread[side:] * spread[side:]
        return carry

    lax.fori_loop(0, modes, forward, 0)
    ratio[...] = amp[0] / (jnp.sqrt(ratio[...]) + SOFTEN)
    terms[...] = jnp.zeros_like(terms)

    def backward(m, carry):
        scale = ratio[...]
        fixed = jnp.concatenate([far[m, :side] * scale, far[m, side:] * scale], axis=1)
        back = first(fwd, fixed)
        back = last(jnp.concatenate([back[:side], back[side:]], axis=1), inv)
        new_real, new_imag = back[:, :side], back[:, side:]
        real, imag = rolled[0, m], rolled[1, m]
        terms[0] += real * new_real + imag * new_imag
        terms[1] += real * new_imag - imag * new_real
        return carry

    lax.fori_loop(0, modes, backward, 0)

    twice[:side, :] = power[...]
    twice[side : 2 * side, :] = power[...]
    twice[2 * side :, :] = jnp.zeros((8, side), jnp.float32)
    lane = lax.broadcasted_iota(jnp.int32, (share, side), 1)
    at = lax.broadcasted_iota(jnp.int32, (share, side), 0) + l * share
    total = jnp.zeros((share, side), jnp.float32)
    there = (None, has_left, has_above, has_left & has_above)
    for group in range(4):
        for layer in range(layers):
            a, b = corner_of(offs, group, layer, side)
            a = jnp.clip(a, 0, side)
            b = jnp.clip(b, 0, side)
            start = side + l * share - a
            extra = lax.rem(start, 8)
            window = twice[pl.ds(pl.multiple_of(start - extra, 8), share + 8), :]
            window = pltpu.roll(window, lax.rem(share + 8 - extra, share + 8), 0)[:share]
            window = pltpu.roll(window, lax.rem(b, side), 1)
            keep = (at < a) if group >= 2 else (at >= a)
            keep &= (lane < b) if group % 2 else (lane >= b)
            if there[group] is not None:
                keep &= there[group]
            total += jnp.where(keep, window, 0.0)
    weight[...] = total + DAMPING


def corner_of(offs, group, layer, side):
    r, c, _ = place()
    tile_row = r - (1 if group >= 2 else 0)
    tile_col = c - (group % 2)
    return offs[group, layer, 0, 0] - tile_row * side, offs[group, layer, 0, 1] - tile_col * side


def sum_kernel(
    sizes, offs, terms, weight, obj, out,
    left, own, lower, upper, shares, s_left, r_left, s_down, r_down, s_rs, r_rs, s_ag, r_ag,
):
    rows, cols, layers = sizes
    share, side = obj.shape[2], obj.shape[3]
    count = s_left.shape[0]
    step = share // count
    r, c, l = place()
    has_right, has_left = c < cols - 1, c > 0
    has_below, has_above = r < rows - 1, r > 0
    parts = [pl.ds(k * step, step) for k in range(count)]
    greet(rows, cols, layers)

    rights, downs, spreads, gathers = [], [], [], []
    for k, part in enumerate(parts):
        rights.append(
            send(
                terms.at[:, :, part], left.at[:, :, part], s_left.at[k], r_left.at[k], (r, c + 1, l)
            )
        )
        downs.append(
            send(
                lower.at[:, :, part], upper.at[:, :, part], s_down.at[k], r_down.at[k], (r + 1, c, l)
            )
        )
        peers = [(d, lax.rem(l + d, layers)) for d in range(1, layers)]
        spreads.append(
            [
                send(
                    own.at[:, peer, part], shares.at[d, :, part],
                    s_rs.at[k, d], r_rs.at[k, d], (r, c, peer),
                )
                for d, peer in peers
            ]
        )
        gathers.append(
            [
                send(
                    out.at[:, l, part], out.at[:, l, part],
                    s_ag.at[k, d], r_ag.at[k, d], (r, c, peer),
                )
                for d, peer in peers
            ]
        )
    for copy in rights:
        pl.when(has_right)(copy.start)

    shape = (layers, step, side)
    lane = lax.broadcasted_iota(jnp.int32, shape, 2)
    line = lax.broadcasted_iota(jnp.int32, shape, 0) * share
    line += lax.broadcasted_iota(jnp.int32, shape, 1)
    down, over = corner_of(offs, 0, l, side)
    left_down, left_over = corner_of(offs, 1, l, side)

    def finish(k):
        part = parts[k]
        for copy in spreads[k]:
            copy.wait_recv()
        for h in range(2):
            number = own[h, l, part, :] + DAMPING * obj[h, l, part, :]
            for d in range(1, layers):
                number += shares[d, h, part, :]
            out[h, l, part, :] = number / weight[part, :]
        for copy in gathers[k]:
            copy.start()

    for k, part in enumerate(parts):
        at = line + k * step
        for h in range(2):
            mine = jnp.where(lane >= over, terms[h, :, part, :], 0.0)
            own[h, :, part, :] = jnp.where(at >= down, mine, 0.0)
            lower[h, :, part, :] = jnp.where(at < down, mine, 0.0)

        @pl.when(has_left)
        def _():
            rights[k].wait_recv()
            for h in range(2):
                other = jnp.where(lane < left_over, left[h, :, part, :], 0.0)
                own[h, :, part, :] += jnp.where(at >= left_down, other, 0.0)
                lower[h, :, part, :] += jnp.where(at < left_down, other, 0.0)

        pl.when(has_below)(downs[k].start)

        @pl.when(jnp.logical_not(has_above))
        def _():
            for copy in spreads[k]:
                copy.start()

    @pl.when(has_above)
    def _():
        for k, part in enumerate(parts):
            downs[k].wait_recv()
            for h in range(2):
                own[h, :, part, :] += upper[h, :, part, :]
            for copy in spreads[k]:
                copy.start()
            if k >= 2:
                finish(k - 2)
        for k in range(max(count - 2, 0), count):
            finish(k)

    @pl.when(jnp.logical_not(has_above))
    def _():
        for k in range(count):
            finish(k)

    for k in range(count):
        for copy in gathers[k]:
            copy.wait()
        for copy in spreads[k]:
            copy.wait_send()

    @pl.when(has_right)
    def _():
        for copy in rights:
            copy.wait_send()

    @pl.when(has_below)
    def _():
        for copy in downs:
            copy.wait_send()


def tables(side):
    steps = np.arange(side)
    angle = (steps[:, None] * steps[None, :] % side) * (2.0 * np.pi / side)
    real, imag = np.cos(angle) / np.sqrt(side), -np.sin(angle) / np.sqrt(side)
    both = np.block([[real, imag], [-imag, real]])

    def halves(x):
        x = x.astype(np.float32)
        high = x.astype(jnp.bfloat16)
        return high, (x - high.astype(np.float32)).astype(jnp.bfloat16)

    return halves(both) + halves(both.T)


def body(sizes, object_field, probe_modes, amplitudes, offsets):
    rows, cols, layers = sizes
    side = object_field.shape[1]
    assert object_field.shape[2] == side and probe_modes.shape[2] == side
    assert offsets.shape[0] == 1 and side % (8 * layers) == 0
    modes = probe_modes.shape[1]
    vmem = pl.BlockSpec(memory_space=pltpu.VMEM)
    smem = pl.BlockSpec(memory_space=pltpu.SMEM)
    pair = (2, side, side)
    f32 = jnp.float32
    dma = pltpu.SemaphoreType.DMA
    merged, offs = pl.pallas_call(
        functools.partial(halo_kernel, sizes),
        out_shape=(
            jax.ShapeDtypeStruct(pair, f32),
            jax.ShapeDtypeStruct((4, layers, 1, 128), jnp.int32),
        ),
        in_specs=[smem, vmem],
        out_specs=(vmem, vmem),
        scratch_shapes=[pltpu.VMEM(pair, f32)] * 3
        + [dma(()), dma(())]
        + [dma((PIECES,))] * 4
        + [dma((layers,))] * 2
        + [dma((3,))] * 2,
        compiler_params=pltpu.CompilerParams(collective_id=0, has_side_effects=True),
        name="halo",
    )(offsets, object_field)
    terms, weight = pl.pallas_call(
        functools.partial(wave_kernel, sizes),
        out_shape=(
            jax.ShapeDtypeStruct(pair, f32),
            jax.ShapeDtypeStruct((side // layers, side), f32),
        ),
        in_specs=[smem, smem] + [vmem] * 7,
        out_specs=(vmem, vmem),
        scratch_shapes=[
            pltpu.VMEM((2, modes, side, side), f32),
            pltpu.VMEM((modes, 2 * side, side), f32),
            pltpu.VMEM((side, side), f32),
            pltpu.VMEM((side, side), f32),
            pltpu.VMEM((2 * side + 8, side), f32),
        ],
        name="wave",
    )(offsets, offs, merged, probe_modes, amplitudes, *(jnp.asarray(t) for t in tables(side)))
    share = side // layers
    count = min(PIECES, share // 8)
    cut = (2, layers, share, side)
    new_object = pl.pallas_call(
        functools.partial(sum_kernel, sizes),
        out_shape=jax.ShapeDtypeStruct(cut, f32),
        in_specs=[smem] + [vmem] * 3,
        out_specs=vmem,
        scratch_shapes=[pltpu.VMEM(cut, f32)] * 4
        + [pltpu.VMEM((layers, 2, share, side), f32)]
        + [dma((count,))] * 4
        + [dma((count, layers))] * 4,
        compiler_params=pltpu.CompilerParams(collective_id=1, has_side_effects=True),
        name="sums",
    )(offs, terms.reshape(cut), weight, object_field.reshape(cut))
    return new_object.reshape(pair)


def solution(mesh):
    sizes = tuple(mesh.shape[a] for a in AXES)
    placed = (
        P(None, "row", "col"),
        P(),
        P(("row", "col", "layer"), None, None),
        P(("row", "col", "layer"), None),
    )
    return jax.shard_map(
        functools.partial(body, sizes),
        mesh=mesh,
        in_specs=placed,
        out_specs=P(None, "row", "col"),
        check_vma=False,
    )
```

```python
import functools

import jax
import jax.numpy as jnp
import numpy as np
from jax import lax
from jax.experimental import pallas as pl
from jax.experimental.pallas import tpu as pltpu
from jax.sharding import PartitionSpec as P

SOFTEN = 0.05
DAMPING = 0.5
AXES = ("row", "col", "layer")
PIECES = 4
LAG = 2


def place():
    return tuple(lax.axis_index(a) for a in AXES)


def send(src, dst, send_sem, recv_sem, device):
    return pltpu.make_async_remote_copy(
        src_ref=src,
        dst_ref=dst,
        send_sem=send_sem,
        recv_sem=recv_sem,
        device_id=device,
        device_id_type=pl.DeviceIdType.MESH,
    )


def greet(rows, cols, layers):
    r, c, l = place()
    barrier = pltpu.get_barrier_semaphore()

    def tell(device):
        pl.semaphore_signal(
            barrier, inc=1, device_id=device, device_id_type=pl.DeviceIdType.MESH
        )

    near = (
        (c > 0, (r, c - 1, l)),
        (c < cols - 1, (r, c + 1, l)),
        (r > 0, (r - 1, c, l)),
        (r < rows - 1, (r + 1, c, l)),
    )
    for there, device in near:
        pl.when(there)(functools.partial(tell, device))
    for d in range(1, layers):
        tell((r, c, lax.rem(l + d, layers)))
    count = layers - 1
    for there, _ in near:
        count += there.astype(jnp.int32)
    pl.semaphore_wait(barrier, count)


def split(x):
    high = x.astype(jnp.bfloat16)
    return high, (x - high.astype(jnp.float32)).astype(jnp.bfloat16)


def prod(left, right):
    def one(a, b):
        return jnp.dot(a, b, preferred_element_type=jnp.float32)

    return one(left[0], right[0]) + (one(left[0], right[1]) + one(left[1], right[0]))


def turned(x, amount, axis):
    length = x.shape[axis]
    bit = 1
    while bit < length:
        x = jnp.where(lax.rem(lax.div(amount, bit), 2) == 1, jnp.roll(x, bit, axis), x)
        bit *= 2
    return x


def corner_of(offs, group, layer, side):
    r, c, _ = place()
    tile_row = r - (1 if group >= 2 else 0)
    tile_col = c - (group % 2)
    return offs[group, layer, 0, 0] - tile_row * side, offs[group, layer, 0, 1] - tile_col * side


def kernel(
    sizes, corner, obj, probe_hbm, amp_hbm, fwd_high_hbm, fwd_low_hbm, inv_high_hbm, inv_low_hbm,
    out,
    probe, amp, fwd_high, fwd_low, inv_high, inv_low, offs, corners,
    right, below, diag, rolled, lines, far, ratio, power, weight, rows_of,
    terms, left, own, lower, upper, shares,
    s_load, s_corner, s_off, r_off, s_pass, r_pass,
    s_right, r_right, s_below, r_below, s_diag, r_diag,
    s_left, r_left, s_down, r_down, s_rs, r_rs, s_ag, r_ag,
):
    rows, cols, layers = sizes
    share, side = obj.shape[2], obj.shape[3]
    modes = probe.shape[1]
    count = s_left.shape[0]
    step = share // count
    tall = layers * step
    r, c, l = place()
    has_right, has_left = c < cols - 1, c > 0
    has_below, has_above = r < rows - 1, r > 0
    parts = [pl.ds(k * step, step) for k in range(count)]
    down = corner[0, 0] - r * side
    over = corner[0, 1] - c * side
    loads = [
        pltpu.make_async_copy(src, dst, s_load.at[i])
        for i, (src, dst) in enumerate(
            (
                (probe_hbm, probe),
                (fwd_high_hbm, fwd_high),
                (fwd_low_hbm, fwd_low),
                (inv_high_hbm, inv_high),
                (inv_low_hbm, inv_low),
                (amp_hbm, amp),
            )
        )
    ]
    for copy in loads:
        copy.start()
    at = lax.broadcasted_iota(jnp.int32, (1, 1, 128), 2)
    offs[0, pl.ds(l, 1)] = jnp.where(at == 0, corner[0, 0], corner[0, 1])
    greet(rows, cols, layers)

    west, east = (r, c - 1, l), (r, c + 1, l)
    north, south = (r - 1, c, l), (r + 1, c, l)

    def pieces(src, dst, sems, device):
        return [
            send(src.at[:, :, part], dst.at[:, :, part], sems[0].at[k], sems[1].at[k], device)
            for k, part in enumerate(parts)
        ]

    lefts = pieces(obj, right, (s_right, r_right), west)
    ups = pieces(obj, below, (s_below, r_below), north)
    diags = pieces(below, diag, (s_diag, r_diag), west)
    for k in range(count):
        pl.when(has_left)(lefts[k].start)
        pl.when(has_above)(ups[k].start)
    mine = offs.at[0, pl.ds(l, 1)]
    around = [(d, lax.rem(l + d, layers)) for d in range(1, layers)]
    peers = [send(mine, mine, s_off.at[d], r_off.at[d], (r, c, p)) for d, p in around]
    for peer in peers:
        peer.start()
    loads[0].wait()

    def forward(k):
        @pl.when(has_below)
        def _():
            ups[k].wait_recv()
            pl.when(has_left)(diags[k].start)

    def prepare(m):
        for h in range(2):
            x = probe[h, m].reshape(side, side)
            rolled[h, m] = turned(turned(x, down, 0), over, 1).reshape(layers, share, side)

    power[...] = jnp.zeros_like(power)
    for k in range(max(modes, count)):
        if k < modes:
            prepare(k)
            real, imag = probe[0, k], probe[1, k]
            power[...] += (real * real + imag * imag).reshape(side, side)
        if k == 0:
            for peer in peers:
                peer.wait()
            across = send(offs.at[0], offs.at[1], s_pass.at[0], r_pass.at[0], east)
            pl.when(has_right)(across.start)
        if k < count:
            forward(k)

    down0 = send(offs.at[0], offs.at[2], s_pass.at[1], r_pass.at[1], south)
    down1 = send(offs.at[1], offs.at[3], s_pass.at[2], r_pass.at[2], south)
    pl.when(has_left)(across.wait_recv)

    @pl.when(has_below)
    def _():
        down0.start()
        pl.when(has_left)(down1.start)

    for copy in loads[1:]:
        copy.wait()
    fwd, inv = (fwd_high, fwd_low), (inv_high, inv_low)

    def last(x, table):
        return prod(split(x), (table[0][...], table[1][...]))

    def first(table, x):
        a = (table[0][:, :side], table[1][:, :side])
        b = (table[0][:, side:], table[1][:, side:])
        return prod(a, split(x[:, :side])) + prod(b, split(x[:, side:]))

    shape = (layers, step, side)
    lane = lax.broadcasted_iota(jnp.int32, shape, 2)
    line = lax.broadcasted_iota(jnp.int32, shape, 0) * share
    line += lax.broadcasted_iota(jnp.int32, shape, 1)

    for k, part in enumerate(parts):
        high = line + k * step < down
        for h in range(2):
            own[h, :, part, :] = obj[h, :, part, :]

        @pl.when(has_right)
        def _():
            lefts[k].wait_recv()
            for h in range(2):
                own[h, :, part, :] = jnp.where(
                    lane < over, right[h, :, part, :], own[h, :, part, :]
                )

        @pl.when(has_below)
        def _():
            for h in range(2):
                own[h, :, part, :] = jnp.where(
                    high & (lane >= over), below[h, :, part, :], own[h, :, part, :]
                )

        @pl.when(has_below & has_right)
        def _():
            diags[k].wait_recv()
            for h in range(2):
                own[h, :, part, :] = jnp.where(
                    high & (lane < over), diag[h, :, part, :], own[h, :, part, :]
                )

        patch = [own[h, :, part, :].reshape(tall, side) for h in range(2)]
        waves = []
        for m in range(modes):
            real, imag = (rolled[h, m, :, part, :].reshape(tall, side) for h in range(2))
            waves.append(
                jnp.concatenate(
                    [real * patch[0] - imag * patch[1], real * patch[1] + imag * patch[0]], axis=1
                )
            )
        half = last(jnp.concatenate(waves, axis=0), fwd)
        for m in range(modes):
            lines[m, :, part, :] = half[m * tall : (m + 1) * tall].reshape(layers, step, 2 * side)

    ratio[...] = jnp.zeros_like(ratio)

    def columns(m, carry):
        spread = first(inv, lines[m].reshape(side, 2 * side))
        far[m] = spread
        ratio[...] += spread[:side] * spread[:side] + spread[side:] * spread[side:]
        return carry

    lax.fori_loop(0, modes, columns, 0)
    ratio[...] = amp[0] / (jnp.sqrt(ratio[...]) + SOFTEN)

    def back(m, carry):
        scale = ratio[...]
        fixed = jnp.concatenate([far[m, :side] * scale, far[m, side:] * scale], axis=1)
        x = first(fwd, fixed)
        x = jnp.concatenate([x[:side], x[side:]], axis=1)
        lines[m] = x.reshape(layers, share, 2 * side)
        return carry

    lax.fori_loop(0, modes, back, 0)

    pl.when(has_above)(down0.wait_recv)
    pl.when(has_above & has_left)(down1.wait_recv)

    @pl.when(jnp.logical_not(has_left))
    def _():
        offs[1] = jnp.zeros(offs.shape[1:], jnp.int32)

    @pl.when(jnp.logical_not(has_above))
    def _():
        offs[2] = jnp.zeros(offs.shape[1:], jnp.int32)

    @pl.when(jnp.logical_not(has_above & has_left))
    def _():
        offs[3] = jnp.zeros(offs.shape[1:], jnp.int32)

    fetch = pltpu.make_async_copy(offs, corners, s_corner)
    fetch.start()
    fetch.wait()

    rights = pieces(terms, left, (s_left, r_left), east)
    downs = pieces(lower, upper, (s_down, r_down), south)
    spreads, gathers = [], []
    for k, part in enumerate(parts):
        spreads.append(
            [
                send(
                    own.at[:, p, part], shares.at[d, :, part],
                    s_rs.at[k, d], r_rs.at[k, d], (r, c, p),
                )
                for d, p in around
            ]
        )
        gathers.append(
            [
                send(
                    out.at[:, l, part], out.at[:, l, part],
                    s_ag.at[k, d], r_ag.at[k, d], (r, c, p),
                )
                for d, p in around
            ]
        )
    left_down, left_over = corner_of(corners, 1, l, side)

    def rows_back(k):
        part = parts[k]
        x = jnp.concatenate(
            [lines[m, :, part, :].reshape(tall, 2 * side) for m in range(modes)], axis=0
        )
        x = last(x, inv)
        sums = [jnp.zeros((tall, side), jnp.float32)] * 2
        for m in range(modes):
            new_real = x[m * tall : (m + 1) * tall, :side]
            new_imag = x[m * tall : (m + 1) * tall, side:]
            real, imag = (rolled[h, m, :, part, :].reshape(tall, side) for h in range(2))
            sums[0] += real * new_real + imag * new_imag
            sums[1] += real * new_imag - imag * new_real
        for h in range(2):
            terms[h, :, part, :] = sums[h].reshape(layers, step, side)
        pl.when(has_right)(rights[k].start)

    def share_out(k):
        part = parts[k]
        at = line + k * step
        for h in range(2):
            mine = jnp.where(lane >= over, terms[h, :, part, :], 0.0)
            own[h, :, part, :] = jnp.where(at >= down, mine, 0.0)
            lower[h, :, part, :] = jnp.where(at < down, mine, 0.0)

        @pl.when(has_left)
        def _():
            rights[k].wait_recv()
            for h in range(2):
                other = jnp.where(lane < left_over, left[h, :, part, :], 0.0)
                own[h, :, part, :] += jnp.where(at >= left_down, other, 0.0)
                lower[h, :, part, :] += jnp.where(at < left_down, other, 0.0)

        pl.when(has_below)(downs[k].start)

        @pl.when(jnp.logical_not(has_above))
        def _():
            for copy in spreads[k]:
                copy.start()

    def finish(k):
        part = parts[k]
        for copy in spreads[k]:
            copy.wait_recv()
        for h in range(2):
            number = own[h, l, part, :] + DAMPING * obj[h, l, part, :]
            for d in range(1, layers):
                number += shares[d, h, part, :]
            out[h, l, part, :] = number / weight[part, :]
        for copy in gathers[k]:
            copy.start()

    for k in range(count + LAG):
        if k < count:
            rows_back(k)
        if k >= LAG:
            share_out(k - LAG)

    across_share = lax.broadcasted_iota(jnp.int32, (share, side), 1)
    along_share = lax.broadcasted_iota(jnp.int32, (share, side), 0) + l * share
    weight[...] = jnp.full_like(weight, DAMPING)
    there = (None, has_left, has_above, has_left & has_above)
    for group in range(4):

        def add(layer, carry, group=group):
            a, b = corner_of(corners, group, layer, side)
            window = turned(power[...], a, 0).reshape(layers, share, side)
            rows_of[...] = window
            window = rows_of[l]
            window = turned(window, b, 1)
            keep = (along_share < a) if group >= 2 else (along_share >= a)
            keep &= (across_share < b) if group % 2 else (across_share >= b)
            weight[...] += jnp.where(keep, window, 0.0)
            return carry

        def all_layers(add=add):
            lax.fori_loop(0, layers, add, 0)

        if there[group] is None:
            all_layers()
        else:
            pl.when(there[group])(all_layers)

    @pl.when(has_above)
    def _():
        for k, part in enumerate(parts):
            downs[k].wait_recv()
            for h in range(2):
                own[h, :, part, :] += upper[h, :, part, :]
            for copy in spreads[k]:
                copy.start()
            if k >= 2:
                finish(k - 2)
        for k in range(max(count - 2, 0), count):
            finish(k)

    @pl.when(jnp.logical_not(has_above))
    def _():
        for k in range(count):
            finish(k)

    for k in range(count):
        for copy in gathers[k]:
            copy.wait()
        for copy in spreads[k]:
            copy.wait_send()

    @pl.when(has_left)
    def _():
        for copy in lefts:
            copy.wait_send()

    @pl.when(has_above)
    def _():
        for copy in ups:
            copy.wait_send()

    @pl.when(has_right)
    def _():
        across.wait_send()
        for copy in rights:
            copy.wait_send()

    @pl.when(has_below)
    def _():
        down0.wait_send()
        for copy in downs:
            copy.wait_send()

    @pl.when(has_below & has_left)
    def _():
        down1.wait_send()
        for copy in diags:
            copy.wait_send()


def tables(side):
    steps = np.arange(side)
    angle = (steps[:, None] * steps[None, :] % side) * (2.0 * np.pi / side)
    real, imag = np.cos(angle) / np.sqrt(side), -np.sin(angle) / np.sqrt(side)
    both = np.block([[real, imag], [-imag, real]])

    def halves(x):
        x = x.astype(np.float32)
        high = x.astype(jnp.bfloat16)
        return high, (x - high.astype(np.float32)).astype(jnp.bfloat16)

    return halves(both) + halves(both.T)


def body(sizes, object_field, probe_modes, amplitudes, offsets):
    rows, cols, layers = sizes
    side = object_field.shape[1]
    assert object_field.shape[2] == side and probe_modes.shape[2] == side
    assert offsets.shape[0] == 1 and side % (8 * layers) == 0
    modes = probe_modes.shape[1]
    vmem = pl.BlockSpec(memory_space=pltpu.VMEM)
    smem = pl.BlockSpec(memory_space=pltpu.SMEM)
    pair = (2, side, side)
    f32 = jnp.float32
    dma = pltpu.SemaphoreType.DMA
    share = side // layers
    count = min(PIECES, share // 8)
    cut = (2, layers, share, side)
    tabs = tuple(jnp.asarray(t) for t in tables(side))
    tab = pltpu.VMEM((2 * side, 2 * side), jnp.bfloat16)
    probe_cut = (2, modes, layers, share, side)
    whole = pltpu.VMEM(cut, f32)
    corners = (4, layers, 1, 128)
    new_object = pl.pallas_call(
        functools.partial(kernel, sizes),
        out_shape=jax.ShapeDtypeStruct(cut, f32),
        in_specs=[smem, vmem] + [pl.BlockSpec(memory_space=pl.ANY)] * 6,
        out_specs=vmem,
        scratch_shapes=[pltpu.VMEM(probe_cut, f32), pltpu.VMEM((1, side, side), f32)]
        + [tab] * 4
        + [pltpu.VMEM(corners, jnp.int32), pltpu.SMEM(corners, jnp.int32)]
        + [whole] * 3
        + [
            pltpu.VMEM(probe_cut, f32),
            pltpu.VMEM((modes, layers, share, 2 * side), f32),
            pltpu.VMEM((modes, 2 * side, side), f32),
            pltpu.VMEM((side, side), f32),
            pltpu.VMEM((side, side), f32),
            pltpu.VMEM((share, side), f32),
            pltpu.VMEM(cut[1:], f32),
        ]
        + [whole] * 5
        + [pltpu.VMEM((layers, 2, share, side), f32)]
        + [dma((6,)), dma(())]
        + [dma((layers,))] * 2
        + [dma((3,))] * 2
        + [dma((count,))] * 10
        + [dma((count, layers))] * 4,
        compiler_params=pltpu.CompilerParams(
            collective_id=0, has_side_effects=True, vmem_limit_bytes=60 * 1024 * 1024
        ),
        name="update",
    )(
        offsets,
        object_field.reshape(cut),
        probe_modes.reshape(probe_cut),
        amplitudes,
        *tabs,
    )
    return new_object.reshape(pair)


def solution(mesh):
    sizes = tuple(mesh.shape[a] for a in AXES)
    placed = (
        P(None, "row", "col"),
        P(),
        P(("row", "col", "layer"), None, None),
        P(("row", "col", "layer"), None),
    )
    return jax.shard_map(
        functools.partial(body, sizes),
        mesh=mesh,
        in_specs=placed,
        out_specs=P(None, "row", "col"),
        check_vma=False,
    )
```

```python
import functools

import jax
import jax.numpy as jnp
import numpy as np
from jax import lax
from jax.experimental import pallas as pl
from jax.experimental.pallas import tpu as pltpu
from jax.sharding import PartitionSpec as P

SOFTEN = 0.05
DAMPING = 0.5
AXES = ("row", "col", "layer")
PIECES = 4
LAG = 2


def place():
    return tuple(lax.axis_index(a) for a in AXES)


def send(src, dst, send_sem, recv_sem, device):
    return pltpu.make_async_remote_copy(
        src_ref=src,
        dst_ref=dst,
        send_sem=send_sem,
        recv_sem=recv_sem,
        device_id=device,
        device_id_type=pl.DeviceIdType.MESH,
    )


def greet(rows, cols, layers):
    r, c, l = place()
    barrier = pltpu.get_barrier_semaphore()

    def tell(device):
        pl.semaphore_signal(
            barrier, inc=1, device_id=device, device_id_type=pl.DeviceIdType.MESH
        )

    near = (
        (c > 0, (r, c - 1, l)),
        (c < cols - 1, (r, c + 1, l)),
        (r > 0, (r - 1, c, l)),
        (r < rows - 1, (r + 1, c, l)),
    )
    for there, device in near:
        pl.when(there)(functools.partial(tell, device))
    for d in range(1, layers):
        tell((r, c, lax.rem(l + d, layers)))
    count = layers - 1
    for there, _ in near:
        count += there.astype(jnp.int32)
    pl.semaphore_wait(barrier, count)


def split(x):
    high = x.astype(jnp.bfloat16)
    return high, (x - high.astype(jnp.float32)).astype(jnp.bfloat16)


def prod(left, right):
    def one(a, b):
        return jnp.dot(a, b, preferred_element_type=jnp.float32)

    return one(left[0], right[0]) + (one(left[0], right[1]) + one(left[1], right[0]))


def turned(x, amount, axis):
    return pltpu.roll(x, amount, axis)


def corner_of(offs, group, layer, side):
    r, c, _ = place()
    tile_row = r - (1 if group >= 2 else 0)
    tile_col = c - (group % 2)
    return offs[group, layer, 0, 0] - tile_row * side, offs[group, layer, 0, 1] - tile_col * side


def kernel(
    sizes, corner, obj, probe_hbm, amp_hbm, fwd_high_hbm, fwd_low_hbm, inv_high_hbm, inv_low_hbm,
    out,
    probe, amp, fwd_high, fwd_low, inv_high, inv_low, offs, corners,
    right, below, diag, rolled, lines, far, ratio, power, weight, rows_of,
    terms, left, own, lower, upper, shares,
    s_load, s_corner, s_off, r_off, s_pass, r_pass,
    s_right, r_right, s_below, r_below, s_diag, r_diag,
    s_left, r_left, s_down, r_down, s_rs, r_rs, s_ag, r_ag,
):
    rows, cols, layers = sizes
    share, side = obj.shape[2], obj.shape[3]
    modes = probe.shape[1]
    count = s_left.shape[0]
    step = share // count
    tall = layers * step
    r, c, l = place()
    has_right, has_left = c < cols - 1, c > 0
    has_below, has_above = r < rows - 1, r > 0
    parts = [pl.ds(k * step, step) for k in range(count)]
    down = corner[0, 0] - r * side
    over = corner[0, 1] - c * side
    loads = [
        pltpu.make_async_copy(src, dst, s_load.at[i])
        for i, (src, dst) in enumerate(
            (
                (probe_hbm, probe),
                (fwd_high_hbm, fwd_high),
                (fwd_low_hbm, fwd_low),
                (inv_high_hbm, inv_high),
                (inv_low_hbm, inv_low),
                (amp_hbm, amp),
            )
        )
    ]
    for copy in loads:
        copy.start()
    at = lax.broadcasted_iota(jnp.int32, (1, 1, 128), 2)
    offs[0, pl.ds(l, 1)] = jnp.where(at == 0, corner[0, 0], corner[0, 1])
    greet(rows, cols, layers)

    west, east = (r, c - 1, l), (r, c + 1, l)
    north, south = (r - 1, c, l), (r + 1, c, l)

    def pieces(src, dst, sems, device):
        return [
            send(src.at[:, :, part], dst.at[:, :, part], sems[0].at[k], sems[1].at[k], device)
            for k, part in enumerate(parts)
        ]

    lefts = pieces(obj, right, (s_right, r_right), west)
    ups = pieces(obj, below, (s_below, r_below), north)
    diags = pieces(below, diag, (s_diag, r_diag), west)
    for k in range(count):
        pl.when(has_left)(lefts[k].start)
        pl.when(has_above)(ups[k].start)
    mine = offs.at[0, pl.ds(l, 1)]
    around = [(d, lax.rem(l + d, layers)) for d in range(1, layers)]
    peers = [send(mine, mine, s_off.at[d], r_off.at[d], (r, c, p)) for d, p in around]
    for peer in peers:
        peer.start()
    loads[0].wait()

    def forward(k):
        @pl.when(has_below)
        def _():
            ups[k].wait_recv()
            pl.when(has_left)(diags[k].start)

    def prepare(m):
        for h in range(2):
            x = probe[h, m].reshape(side, side)
            rolled[h, m] = turned(turned(x, down, 0), over, 1).reshape(layers, share, side)

    power[...] = jnp.zeros_like(power)
    for k in range(max(modes, count)):
        if k < modes:
            prepare(k)
            real, imag = probe[0, k], probe[1, k]
            power[...] += (real * real + imag * imag).reshape(side, side)
        if k == 0:
            for peer in peers:
                peer.wait()
            across = send(offs.at[0], offs.at[1], s_pass.at[0], r_pass.at[0], east)
            pl.when(has_right)(across.start)
        if k < count:
            forward(k)

    down0 = send(offs.at[0], offs.at[2], s_pass.at[1], r_pass.at[1], south)
    down1 = send(offs.at[1], offs.at[3], s_pass.at[2], r_pass.at[2], south)
    pl.when(has_left)(across.wait_recv)

    @pl.when(has_below)
    def _():
        down0.start()
        pl.when(has_left)(down1.start)

    for copy in loads[1:]:
        copy.wait()
    fwd, inv = (fwd_high, fwd_low), (inv_high, inv_low)

    def last(x, table):
        return prod(split(x), (table[0][...], table[1][...]))

    def first(table, x):
        a = (table[0][:, :side], table[1][:, :side])
        b = (table[0][:, side:], table[1][:, side:])
        return prod(a, split(x[:, :side])) + prod(b, split(x[:, side:]))

    shape = (layers, step, side)
    lane = lax.broadcasted_iota(jnp.int32, shape, 2)
    line = lax.broadcasted_iota(jnp.int32, shape, 0) * share
    line += lax.broadcasted_iota(jnp.int32, shape, 1)

    for k, part in enumerate(parts):
        high = line + k * step < down
        for h in range(2):
            own[h, :, part, :] = obj[h, :, part, :]

        @pl.when(has_right)
        def _():
            lefts[k].wait_recv()
            for h in range(2):
                own[h, :, part, :] = jnp.where(
                    lane < over, right[h, :, part, :], own[h, :, part, :]
                )

        @pl.when(has_below)
        def _():
            for h in range(2):
                own[h, :, part, :] = jnp.where(
                    high & (lane >= over), below[h, :, part, :], own[h, :, part, :]
                )

        @pl.when(has_below & has_right)
        def _():
            diags[k].wait_recv()
            for h in range(2):
                own[h, :, part, :] = jnp.where(
                    high & (lane < over), diag[h, :, part, :], own[h, :, part, :]
                )

        patch = [own[h, :, part, :].reshape(tall, side) for h in range(2)]
        waves = []
        for m in range(modes):
            real, imag = (rolled[h, m, :, part, :].reshape(tall, side) for h in range(2))
            waves.append(
                jnp.concatenate(
                    [real * patch[0] - imag * patch[1], real * patch[1] + imag * patch[0]], axis=1
                )
            )
        half = last(jnp.concatenate(waves, axis=0), fwd)
        for m in range(modes):
            lines[m, :, part, :] = half[m * tall : (m + 1) * tall].reshape(layers, step, 2 * side)

    ratio[...] = jnp.zeros_like(ratio)

    def columns(m, carry):
        spread = first(inv, lines[m].reshape(side, 2 * side))
        far[m] = spread
        ratio[...] += spread[:side] * spread[:side] + spread[side:] * spread[side:]
        return carry

    lax.fori_loop(0, modes, columns, 0)
    ratio[...] = amp[0] / (jnp.sqrt(ratio[...]) + SOFTEN)

    def back(m, carry):
        scale = ratio[...]
        fixed = jnp.concatenate([far[m, :side] * scale, far[m, side:] * scale], axis=1)
        x = first(fwd, fixed)
        x = jnp.concatenate([x[:side], x[side:]], axis=1)
        lines[m] = x.reshape(layers, share, 2 * side)
        return carry

    lax.fori_loop(0, modes, back, 0)

    pl.when(has_above)(down0.wait_recv)
    pl.when(has_above & has_left)(down1.wait_recv)

    @pl.when(jnp.logical_not(has_left))
    def _():
        offs[1] = jnp.zeros(offs.shape[1:], jnp.int32)

    @pl.when(jnp.logical_not(has_above))
    def _():
        offs[2] = jnp.zeros(offs.shape[1:], jnp.int32)

    @pl.when(jnp.logical_not(has_above & has_left))
    def _():
        offs[3] = jnp.zeros(offs.shape[1:], jnp.int32)

    fetch = pltpu.make_async_copy(offs, corners, s_corner)
    fetch.start()
    fetch.wait()

    rights = pieces(terms, left, (s_left, r_left), east)
    downs = pieces(lower, upper, (s_down, r_down), south)
    spreads, gathers = [], []
    for k, part in enumerate(parts):
        spreads.append(
            [
                send(
                    own.at[:, p, part], shares.at[d, :, part],
                    s_rs.at[k, d], r_rs.at[k, d], (r, c, p),
                )
                for d, p in around
            ]
        )
        gathers.append(
            [
                send(
                    out.at[:, l, part], out.at[:, l, part],
                    s_ag.at[k, d], r_ag.at[k, d], (r, c, p),
                )
                for d, p in around
            ]
        )
    left_down, left_over = corner_of(corners, 1, l, side)

    def rows_back(k):
        part = parts[k]
        x = jnp.concatenate(
            [lines[m, :, part, :].reshape(tall, 2 * side) for m in range(modes)], axis=0
        )
        x = last(x, inv)
        sums = [jnp.zeros((tall, side), jnp.float32)] * 2
        for m in range(modes):
            new_real = x[m * tall : (m + 1) * tall, :side]
            new_imag = x[m * tall : (m + 1) * tall, side:]
            real, imag = (rolled[h, m, :, part, :].reshape(tall, side) for h in range(2))
            sums[0] += real * new_real + imag * new_imag
            sums[1] += real * new_imag - imag * new_real
        for h in range(2):
            terms[h, :, part, :] = sums[h].reshape(layers, step, side)
        pl.when(has_right)(rights[k].start)

    def share_out(k):
        part = parts[k]
        at = line + k * step
        for h in range(2):
            mine = jnp.where(lane >= over, terms[h, :, part, :], 0.0)
            own[h, :, part, :] = jnp.where(at >= down, mine, 0.0)
            lower[h, :, part, :] = jnp.where(at < down, mine, 0.0)

        @pl.when(has_left)
        def _():
            rights[k].wait_recv()
            for h in range(2):
                other = jnp.where(lane < left_over, left[h, :, part, :], 0.0)
                own[h, :, part, :] += jnp.where(at >= left_down, other, 0.0)
                lower[h, :, part, :] += jnp.where(at < left_down, other, 0.0)

        pl.when(has_below)(downs[k].start)

        @pl.when(jnp.logical_not(has_above))
        def _():
            for copy in spreads[k]:
                copy.start()

    def finish(k):
        part = parts[k]
        for copy in spreads[k]:
            copy.wait_recv()
        for h in range(2):
            number = own[h, l, part, :] + DAMPING * obj[h, l, part, :]
            for d in range(1, layers):
                number += shares[d, h, part, :]
            out[h, l, part, :] = number / weight[part, :]
        for copy in gathers[k]:
            copy.start()

    for k in range(count + LAG):
        if k < count:
            rows_back(k)
        if k >= LAG:
            share_out(k - LAG)

    across_share = lax.broadcasted_iota(jnp.int32, (share, side), 1)
    along_share = lax.broadcasted_iota(jnp.int32, (share, side), 0) + l * share
    weight[...] = jnp.full_like(weight, DAMPING)
    there = (None, has_left, has_above, has_left & has_above)
    for group in range(4):

        def add(layer, carry, group=group):
            a, b = corner_of(corners, group, layer, side)
            window = turned(power[...], a, 0).reshape(layers, share, side)
            rows_of[...] = window
            window = rows_of[l]
            window = turned(window, b, 1)
            keep = (along_share < a) if group >= 2 else (along_share >= a)
            keep &= (across_share < b) if group % 2 else (across_share >= b)
            weight[...] += jnp.where(keep, window, 0.0)
            return carry

        def all_layers(add=add):
            lax.fori_loop(0, layers, add, 0)

        if there[group] is None:
            all_layers()
        else:
            pl.when(there[group])(all_layers)

    @pl.when(has_above)
    def _():
        for k, part in enumerate(parts):
            downs[k].wait_recv()
            for h in range(2):
                own[h, :, part, :] += upper[h, :, part, :]
            for copy in spreads[k]:
                copy.start()
            if k >= 2:
                finish(k - 2)
        for k in range(max(count - 2, 0), count):
            finish(k)

    @pl.when(jnp.logical_not(has_above))
    def _():
        for k in range(count):
            finish(k)

    for k in range(count):
        for copy in gathers[k]:
            copy.wait()
        for copy in spreads[k]:
            copy.wait_send()

    @pl.when(has_left)
    def _():
        for copy in lefts:
            copy.wait_send()

    @pl.when(has_above)
    def _():
        for copy in ups:
            copy.wait_send()

    @pl.when(has_right)
    def _():
        across.wait_send()
        for copy in rights:
            copy.wait_send()

    @pl.when(has_below)
    def _():
        down0.wait_send()
        for copy in downs:
            copy.wait_send()

    @pl.when(has_below & has_left)
    def _():
        down1.wait_send()
        for copy in diags:
            copy.wait_send()


def tables(side):
    steps = np.arange(side)
    angle = (steps[:, None] * steps[None, :] % side) * (2.0 * np.pi / side)
    real, imag = np.cos(angle) / np.sqrt(side), -np.sin(angle) / np.sqrt(side)
    both = np.block([[real, imag], [-imag, real]])

    def halves(x):
        x = x.astype(np.float32)
        high = x.astype(jnp.bfloat16)
        return high, (x - high.astype(np.float32)).astype(jnp.bfloat16)

    return halves(both) + halves(both.T)


def body(sizes, object_field, probe_modes, amplitudes, offsets):
    rows, cols, layers = sizes
    side = object_field.shape[1]
    assert object_field.shape[2] == side and probe_modes.shape[2] == side
    assert offsets.shape[0] == 1 and side % (8 * layers) == 0
    modes = probe_modes.shape[1]
    vmem = pl.BlockSpec(memory_space=pltpu.VMEM)
    smem = pl.BlockSpec(memory_space=pltpu.SMEM)
    pair = (2, side, side)
    f32 = jnp.float32
    dma = pltpu.SemaphoreType.DMA
    share = side // layers
    count = min(PIECES, share // 8)
    cut = (2, layers, share, side)
    tabs = tuple(jnp.asarray(t) for t in tables(side))
    tab = pltpu.VMEM((2 * side, 2 * side), jnp.bfloat16)
    probe_cut = (2, modes, layers, share, side)
    whole = pltpu.VMEM(cut, f32)
    corners = (4, layers, 1, 128)
    new_object = pl.pallas_call(
        functools.partial(kernel, sizes),
        out_shape=jax.ShapeDtypeStruct(cut, f32),
        in_specs=[smem, vmem] + [pl.BlockSpec(memory_space=pl.ANY)] * 6,
        out_specs=vmem,
        scratch_shapes=[pltpu.VMEM(probe_cut, f32), pltpu.VMEM((1, side, side), f32)]
        + [tab] * 4
        + [pltpu.VMEM(corners, jnp.int32), pltpu.SMEM(corners, jnp.int32)]
        + [whole] * 3
        + [
            pltpu.VMEM(probe_cut, f32),
            pltpu.VMEM((modes, layers, share, 2 * side), f32),
            pltpu.VMEM((modes, 2 * side, side), f32),
            pltpu.VMEM((side, side), f32),
            pltpu.VMEM((side, side), f32),
            pltpu.VMEM((share, side), f32),
            pltpu.VMEM(cut[1:], f32),
        ]
        + [whole] * 5
        + [pltpu.VMEM((layers, 2, share, side), f32)]
        + [dma((6,)), dma(())]
        + [dma((layers,))] * 2
        + [dma((3,))] * 2
        + [dma((count,))] * 10
        + [dma((count, layers))] * 4,
        compiler_params=pltpu.CompilerParams(
            collective_id=0, has_side_effects=True, vmem_limit_bytes=60 * 1024 * 1024
        ),
        name="update",
    )(
        offsets,
        object_field.reshape(cut),
        probe_modes.reshape(probe_cut),
        amplitudes,
        *tabs,
    )
    return new_object.reshape(pair)


def solution(mesh):
    sizes = tuple(mesh.shape[a] for a in AXES)
    placed = (
        P(None, "row", "col"),
        P(),
        P(("row", "col", "layer"), None, None),
        P(("row", "col", "layer"), None),
    )
    return jax.shard_map(
        functools.partial(body, sizes),
        mesh=mesh,
        in_specs=placed,
        out_specs=P(None, "row", "col"),
        check_vma=False,
    )
```
